32 devices in a mesh: gx: 4 (over y, core), yz: 8 (over z, x).
Axes of the slice: x: 2, y: 2, z: 4, core: 2. Of those that a mesh axis runs over, the one named last changes fastest.
Arguments:
- orbitals: bfloat16 [4, 8, 9, 128, 256], P('gx', 'yz'), may hold values from -0.125 to 0.125
- potential: float32 [4, 8, 256], P('gx', 'yz'), may hold values from 0.25 to 4
- density: bfloat16 [4, 8, 9, 128, 128], P('gx', 'yz'), may hold values from -0.1 to 0.6
- pattern: int32 [4, 8, 9], P('gx', 'yz'), may hold values 0 or 1
Outputs:
- hamiltonian: float32 [4, 8, 9, 128, 128], P('gx', 'yz')
- margin: float32 [4, 8, 9, 128, 128], P('gx', 'yz')
- purified: float32 [4, 8, 9, 128, 128], P('gx', 'yz')
The draws below stay inside these ranges and needn't reach their ends.
All inputs are finite; a program needn't handle non-finite values. No bound on the sum of `pattern` on one device may be relied on, other than what follows from the above.
Results may differ from the reference program's by a relative error of at most 0.0068.
Values may be sent and summed in bfloat16 or wider, within the bound.
A program may use at most 64 MiB of HBM per device.

```python
import math
import jax
import jax.numpy as jnp

BLK = 128
G_DEV = 256
NGX = 4
NYZ = 8


def draw_density(key, part):
    noise = 0.01 * jax.random.normal(key, (NGX, NYZ, 9, BLK, BLK), jnp.float32)
    identity = jnp.eye(BLK, dtype=jnp.float32)
    centre = (jnp.arange(9) == 4).astype(jnp.float32)
    return (noise + 0.5 * centre[None, None, :, None, None] * identity).astype(jnp.bfloat16)


def set_ends(array, rng, low, top_value):
    dims = array.shape
    index_at = [jax.random.randint(jax.random.fold_in(rng, axis), (), 0, dims[axis]) for axis in range(len(dims))]
    array = array.at[tuple(index_at)].set(low)
    longest = dims.index(max(dims))
    index_at[longest] = (index_at[longest] + 1) % dims[longest]
    return array.at[tuple(index_at)].set(top_value)


def block_levels(key, extent, split, least, top_value):
    level = 1.0
    for axis_at, blocks in split:
        heights = jax.random.uniform(jax.random.fold_in(jax.random.fold_in(key, 6), axis_at), (blocks,), jnp.float32, least / len(split), top_value / len(split))
        level = level * jnp.repeat(jnp.exp(heights), extent[axis_at] // blocks).reshape((-1,) + (1,) * (len(extent) - 1 - axis_at))
    return level


def centred(own_key, extent, width, bound, split=(), held_as=jnp.bfloat16):
    gain = block_levels(own_key, extent, split, -0.22, 0.18) if split else 1.0
    result = jax.random.normal(own_key, extent, jnp.float32) * width * gain
    return jnp.minimum(jnp.maximum(result, -bound), bound).astype(held_as)


def setup_inputs(seed: int = 0) -> dict:
    keys = jax.random.split(jax.random.key(seed), 5)
    return {
        "orbitals": centred(keys[0], (NGX, NYZ, 9, BLK, G_DEV), (9 * G_DEV) ** -0.5, 0.125, ((0, 4), (1, 8))),
        "potential": jnp.clip(jnp.exp(math.log(4.0) - 2.7725887 * jax.random.uniform(keys[1], (NGX, NYZ, G_DEV), jnp.float32) ** block_levels(keys[1], (NGX, NYZ, G_DEV), ((0, 4), (1, 8)), -0.2, 0.2)), 0.25, 4.0),
        "density": draw_density(jax.random.fold_in(keys[4], 71), 0),
        "pattern": set_ends((jax.random.randint(keys[3], (NGX, NYZ, 9), 0, 5) < 4).astype(jnp.int32), jax.random.fold_in(keys[3], 1), 0, 1),
    }


def offset_of(index):
    return index // 3 - 1, index % 3 - 1


def slot_for(shift_x, shift_y):
    return (shift_x + 1) * 3 + shift_y + 1


def line_steps(values):
    lead = values.shape[:-1]
    lines = values.astype(jnp.float32).reshape(lead + (values.shape[-1] // 128, 128))
    forward = lines[..., 1:] - lines[..., :-1]
    padded = jnp.concatenate([forward, jnp.zeros(lead + (lines.shape[-2], 1), jnp.float32)], axis=-1)
    return padded.reshape(values.shape).astype(jnp.bfloat16)


def block_product(left, right, keep):
    out = jnp.zeros(left.shape, jnp.float32)
    for first in range(9):
        fa, fb = offset_of(first)
        for second in range(9):
            sa, sb = offset_of(second)
            oa, ob = fa + sa, fb + sb
            if abs(oa) > 1 or abs(ob) > 1:
                continue
            moved = jnp.roll(right[:, :, second], (-fa, -fb), axis=(0, 1))
            term = jnp.einsum("xyij,xyjk->xyik", left[:, :, first].astype(jnp.float32), moved.astype(jnp.float32))
            out = out.at[:, :, slot_for(oa, ob)].add(term)
    return out * keep


def reference(orbitals, potential, density, pattern):
    keep = pattern.astype(jnp.float32)[:, :, :, None, None]
    weighted = (orbitals.astype(jnp.float32) * potential[:, :, None, None, :]).astype(jnp.bfloat16)
    steps = line_steps(orbitals)
    hamiltonian = jnp.zeros(density.shape, jnp.float32)
    margin = jnp.zeros(density.shape, jnp.float32)
    for slot in range(9):
        ka, kb = offset_of(slot)
        left = orbitals[:, :, slot].astype(jnp.float32)
        left_steps = steps[:, :, slot].astype(jnp.float32)
        for target in range(9):
            pa, pb = offset_of(target)
            la, lb = ka - pa, kb - pb
            if abs(la) > 1 or abs(lb) > 1:
                continue
            other = slot_for(la, lb)
            s_term = jnp.einsum("xyig,xyjg->xyij", left, orbitals[:, :, other].astype(jnp.float32))
            h_term = jnp.einsum("xyig,xyjg->xyij", left, weighted[:, :, other].astype(jnp.float32))
            h_term = h_term + 0.5 * jnp.einsum("xyig,xyjg->xyij", left_steps, steps[:, :, other].astype(jnp.float32))
            margin = margin.at[:, :, target].add(jnp.roll(s_term, (-ka, -kb), axis=(0, 1)))
            hamiltonian = hamiltonian.at[:, :, target].add(jnp.roll(h_term, (-ka, -kb), axis=(0, 1)))
    hamiltonian = hamiltonian * keep
    margin = margin * keep
    current = density * pattern.astype(jnp.bfloat16)[:, :, :, None, None]
    margin_low = margin.astype(jnp.bfloat16)
    purified = jnp.zeros(density.shape, jnp.float32)
    for step in range(2):
        first = block_product(current, margin_low, keep)
        first_low = first.astype(jnp.bfloat16)
        third = block_product(first_low, current, keep)
        third_low = third.astype(jnp.bfloat16)
        fifth = block_product(first_low, third_low, keep)
        purified = 3.0 * third - 2.0 * fifth
        current = purified.astype(jnp.bfloat16)
    return hamiltonian, margin, purified
```

```python
import functools

import jax
import jax.numpy as jnp
from jax import lax
from jax.experimental import pallas as pl
from jax.experimental.pallas import tpu as pltpu
from jax.sharding import PartitionSpec as P

MESH = pl.DeviceIdType.MESH
SPAN = (-1, 0, 1)


def part(d):
    return pl.ds(1, 2) if d == 1 else pl.ds(0, 2) if d == -1 else pl.ds(0, 3)


class Halo:
    def __init__(self, where, own, near, send, recv, sign=1, whole=False):
        self.where, self.own, self.near = where, own, near
        self.send, self.recv, self.sign, self.whole = send, recv, sign, whole
        self.direct = {}
        self.passed = {}

    def make(self, src, a, b, da, db, ta, tb, at):
        dst = self.near.at[a, b]
        if not self.whole:
            src = src.at[part(self.sign * da), part(self.sign * db)]
            dst = dst.at[part(self.sign * da), part(self.sign * db)]
        return pltpu.make_async_remote_copy(
            src_ref=src, dst_ref=dst, send_sem=self.send.at[at], recv_sem=self.recv.at[at],
            device_id=self.where(ta, tb), device_id_type=MESH,
        )

    def start(self):
        for at, (da, db) in enumerate(((0, 1), (0, -1), (1, 0), (-1, 0))):
            self.direct[da, db] = self.make(self.own, 1 - da, 1 - db, da, db, da, db, at)
            self.direct[da, db].start()

    def relay(self):
        at = 4
        for db in (1, -1):
            self.direct[0, db].wait_recv()
            for da in (1, -1):
                src = self.near.at[1, 1 - db]
                self.passed[da, db] = self.make(src, 1 - da, 1 - db, da, db, da, 0, at)
                self.passed[da, db].start()
                at += 1

    def finish(self):
        for da in (1, -1):
            self.direct[da, 0].wait_recv()
        for copy in self.passed.values():
            copy.wait_recv()

    def drain(self):
        for copy in list(self.direct.values()) + list(self.passed.values()):
            copy.wait_send()


def product(left, own, near, keep, emit):
    width = left.shape[-1]
    blank = jnp.zeros((width, width), jnp.bfloat16)
    for pa in SPAN:
        total = None
        for fa in SPAN:
            if abs(pa - fa) > 1:
                continue
            lhs = jnp.concatenate([left[fa + 1, fb + 1] for fb in SPAN], axis=1)
            rows = []
            for fb in SPAN:
                src = own if (fa, fb) == (0, 0) else near.at[fa + 1, fb + 1]
                rows.append(jnp.concatenate(
                    [src[pa - fa + 1, pb - fb + 1] if abs(pb - fb) <= 1 else blank for pb in SPAN],
                    axis=1,
                ))
            rhs = jnp.concatenate(rows, axis=0)
            term = jnp.dot(lhs, rhs, preferred_element_type=jnp.float32)
            total = term if total is None else total + term
        for pb in SPAN:
            cut = total[:, (pb + 1) * width:(pb + 2) * width]
            emit(pa + 1, pb + 1, cut * keep[pa + 1, pb + 1])


def overlap(lefts, rights, width, keep, emit):
    for pa in SPAN:
        total = None
        for ka in SPAN:
            if abs(ka - pa) > 1:
                continue
            for kb in SPAN:
                lhs = lefts(ka, kb)
                rhs = rights(ka, kb)
                blank = jnp.zeros(lhs.shape, jnp.bfloat16)
                rows = jnp.concatenate(
                    [rhs[ka - pa + 1, kb - pb + 1] if abs(kb - pb) <= 1 else blank for pb in SPAN],
                    axis=0,
                )
                term = lax.dot_general(
                    lhs, rows, (((1,), (1,)), ((), ())), preferred_element_type=jnp.float32
                )
                total = term if total is None else total + term
        for pb in SPAN:
            cut = total[:, (pb + 1) * width:(pb + 2) * width]
            emit(pa + 1, pb + 1, cut * keep[pa + 1, pb + 1])


def kernel(counts, orb, pot, den, keep, ham, mar, pur,
           o_near, v_near, w_near, d0_near, d1_near, m_near, t0_near, t1_near, first, send, recv):
    width, cells = orb.shape[-2], orb.shape[-1]
    me = (lax.axis_index("gx"), lax.axis_index("yz"))

    def where(da, db):
        return (
            lax.rem(me[0] + da + counts[0], counts[0]),
            lax.rem(me[1] + db + counts[1], counts[1]),
        )

    barrier = pltpu.get_barrier_semaphore()
    for da, db in ((0, 1), (0, -1), (1, 0), (-1, 0)):
        pl.semaphore_signal(barrier, inc=1, device_id=where(da, db), device_id_type=MESH)
    pl.semaphore_wait(barrier, 4)

    used = iter(range(7))

    def halo(own, near, **more):
        at = next(used)
        return Halo(where, own, near, send.at[at], recv.at[at], **more)

    waves = halo(orb, o_near, sign=-1)
    fields = halo(pot, v_near, whole=True)
    waves.start()
    fields.start()
    d_own = d0_near.at[1, 1]
    for a in range(3):
        for b in range(3):
            d_own[a, b] = (den[a, b].astype(jnp.float32) * keep[a, b]).astype(jnp.bfloat16)
    waves.relay()
    fields.relay()
    density = halo(d_own, d0_near)
    density.start()
    waves.finish()

    def region(ka, kb):
        return orb if (ka, kb) == (0, 0) else o_near.at[ka + 1, kb + 1]

    m_own = m_near.at[1, 1]

    def put_margin(a, b, value):
        mar[a, b] = value
        m_own[a, b] = value.astype(jnp.bfloat16)

    overlap(lambda ka, kb: region(ka, kb)[ka + 1, kb + 1], region, width, keep, put_margin)
    margin = halo(m_own, m_near)
    margin.start()
    density.relay()
    fields.finish()

    lane = lax.broadcasted_iota(jnp.int32, (width, 128), 1)
    for ka in SPAN:
        for kb in SPAN:
            src = region(ka, kb)
            field = pot[0] if (ka, kb) == (0, 0) else v_near[ka + 1, kb + 1, 0]
            for la in SPAN:
                for lb in SPAN:
                    if abs(ka - la) > 1 or abs(kb - lb) > 1:
                        continue
                    value = src[la + 1, lb + 1].astype(jnp.float32)
                    dst = w_near.at[ka + 1, kb + 1, la + 1, lb + 1]
                    dst[:, :cells] = (value * field).astype(jnp.bfloat16)
                    for line in range(cells // 128):
                        piece = value[:, line * 128:(line + 1) * 128]
                        ahead = pltpu.roll(piece, 127, 1)
                        step = jnp.where(lane < 127, ahead - piece, 0.0)
                        at = cells + line * 128
                        dst[:, at:at + 128] = step.astype(jnp.bfloat16)
    margin.relay()

    def h_left(ka, kb):
        half = w_near[ka + 1, kb + 1, ka + 1, kb + 1][:, cells:] * 0.5
        return jnp.concatenate([region(ka, kb)[ka + 1, kb + 1], half.astype(jnp.bfloat16)], axis=1)

    def put_ham(a, b, value):
        ham[a, b] = value

    overlap(h_left, lambda ka, kb: w_near.at[ka + 1, kb + 1], width, keep, put_ham)
    margin.finish()
    density.finish()

    def put_first(a, b, value):
        first[a, b] = value.astype(jnp.bfloat16)

    started = [waves, fields, density, margin]
    nears = ((d0_near, t0_near), (d1_near, t1_near))
    for turn, (d_near, t_near) in enumerate(nears):
        d_row, t_row = d_near.at[1, 1], t_near.at[1, 1]
        product(d_row, m_own, m_near, keep, put_first)
        if turn:
            rows.relay()
            rows.finish()

        def put_third(a, b, value):
            pur[a, b] = 3.0 * value
            t_row[a, b] = value.astype(jnp.bfloat16)

        product(first, d_row, d_near, keep, put_third)
        cubic = halo(t_row, t_near)
        cubic.start()
        cubic.relay()
        cubic.finish()
        started.append(cubic)
        after = nears[turn + 1][0].at[1, 1] if turn + 1 < len(nears) else None

        def put_fifth(a, b, value):
            result = pur[a, b] - 2.0 * value
            pur[a, b] = result
            if after is not None:
                after[a, b] = result.astype(jnp.bfloat16)

        product(first, t_row, t_near, keep, put_fifth)
        if after is not None:
            rows = halo(after, nears[turn + 1][0])
            rows.start()
            started.append(rows)
    for one in started:
        one.drain()


def body(counts, orbitals, potential, density, pattern):
    width, cells = orbitals.shape[3], orbitals.shape[4]
    keep = jnp.broadcast_to(
        pattern.reshape(3, 3, 1, 1).astype(jnp.float32), (3, 3, 1, 128)
    )
    near = pltpu.VMEM((3, 3, 3, 3, width, width), jnp.bfloat16)
    blocks = jax.ShapeDtypeStruct((3, 3, width, width), jnp.float32)
    vmem = pl.BlockSpec(memory_space=pltpu.VMEM)
    outs = pl.pallas_call(
        functools.partial(kernel, counts),
        out_shape=(blocks,) * 3,
        in_specs=[vmem] * 4,
        out_specs=(vmem,) * 3,
        scratch_shapes=[
            pltpu.VMEM((3, 3, 3, 3, width, cells), jnp.bfloat16),
            pltpu.VMEM((3, 3, 1, 1, cells), jnp.float32),
            pltpu.VMEM((3, 3, 3, 3, width, 2 * cells), jnp.bfloat16),
            near, near, near, near, near,
            pltpu.VMEM((3, 3, width, width), jnp.bfloat16),
            pltpu.SemaphoreType.DMA((7, 8)),
            pltpu.SemaphoreType.DMA((7, 8)),
        ],
        compiler_params=pltpu.CompilerParams(
            collective_id=0, has_side_effects=True, vmem_limit_bytes=60 * 2**20
        ),
    )(
        orbitals.reshape(3, 3, width, cells),
        potential.reshape(1, 1, cells),
        density.reshape(3, 3, width, width),
        keep,
    )
    return tuple(out.reshape(1, 1, 9, width, width) for out in outs)


def solution(mesh):
    rows = P("gx", "yz", None, None, None)
    flat = P("gx", "yz", None)
    return jax.shard_map(
        functools.partial(body, (mesh.shape["gx"], mesh.shape["yz"])),
        mesh=mesh,
        in_specs=(rows, flat, rows, flat),
        out_specs=(rows,) * 3,
        check_vma=False,
    )
```

```python
import functools

import jax
import jax.numpy as jnp
from jax import lax
from jax.experimental import pallas as pl
from jax.experimental.pallas import tpu as pltpu
from jax.sharding import PartitionSpec as P

MESH = pl.DeviceIdType.MESH
SPAN = (-1, 0, 1)


def part(d):
    return pl.ds(1, 2) if d == 1 else pl.ds(0, 2) if d == -1 else pl.ds(0, 3)


class Halo:
    def __init__(self, where, own, near, send, recv, sign=1, whole=False, slim=False):
        self.where, self.own, self.near = where, own, near
        self.send, self.recv, self.sign, self.whole, self.slim = send, recv, sign, whole, slim
        outer = 2 * lax.rem(lax.axis_index("gx"), 2) - 1
        self.order = [
            (db, piece, pa, das)
            for piece, pa, das in (
                ((0, None, (1, -1)),) if whole else
                ((0, 1, (1, -1)), (1, 0, ()), (2, 2, ())) if slim else (
                    (0, 1, (outer, -outer)),
                    (1, 1 + sign * outer, (outer,)),
                    (2, 1 - sign * outer, (-outer,)),
                )
            )
            for db in (1, -1)
        ]
        self.direct = {}
        self.passed = []
        self.next = 0

    def make(self, src, da, db, ta, tb, pa, pb=None):
        dst = self.near.at[1 - da, 1 - db]
        if not self.whole:
            pb = part(self.sign * db) if pb is None else pb
            src = src.at[pa, pb]
            dst = dst.at[pa, pb]
        at = self.next
        self.next += 1
        copy = pltpu.make_async_remote_copy(
            src_ref=src, dst_ref=dst, send_sem=self.send.at[at], recv_sem=self.recv.at[at],
            device_id=self.where(ta, tb), device_id_type=MESH,
        )
        copy.start()
        return copy

    def start_far(self):
        for db, piece, pa, _ in self.order:
            self.direct[db, piece] = self.make(self.own, 0, db, 0, db, pa)

    def start_near(self):
        for da in (1, -1):
            pa = 1 if self.slim else part(self.sign * da)
            self.direct[da] = self.make(self.own, da, 0, da, 0, pa)

    def start(self):
        self.start_far()
        self.start_near()

    def relay(self):
        for db, piece, pa, das in self.order:
            if das:
                self.direct[db, piece].wait_recv()
            for da in das:
                src = self.near.at[1, 1 - db]
                pb = 1 if self.slim else None
                self.passed.append(self.make(src, da, db, da, 0, pa, pb))

    def finish(self):
        for db, piece, _, das in self.order:
            if not das:
                self.direct[db, piece].wait_recv()
        for da in (1, -1):
            self.direct[da].wait_recv()
        for copy in self.passed:
            copy.wait_recv()

    def drain(self):
        for copy in list(self.direct.values()) + self.passed:
            copy.wait_send()


def product(left, own, near, keep, emit):
    width = left.shape[-1]
    blank = jnp.zeros((width, width), jnp.bfloat16)
    for pa in SPAN:
        total = None
        for fa in SPAN:
            if abs(pa - fa) > 1:
                continue
            lhs = jnp.concatenate([left[fa + 1, fb + 1] for fb in SPAN], axis=1)
            rows = []
            for fb in SPAN:
                src = own if (fa, fb) == (0, 0) else near.at[fa + 1, fb + 1]
                rows.append(jnp.concatenate(
                    [src[pa - fa + 1, pb - fb + 1] if abs(pb - fb) <= 1 else blank for pb in SPAN],
                    axis=1,
                ))
            rhs = jnp.concatenate(rows, axis=0)
            term = jnp.dot(lhs, rhs, preferred_element_type=jnp.float32)
            total = term if total is None else total + term
        for pb in SPAN:
            cut = total[:, (pb + 1) * width:(pb + 2) * width]
            emit(pa + 1, pb + 1, cut * keep[pa + 1, pb + 1])


def overlap(lefts, rights, width, emit):
    for pa in SPAN:
        total = None
        for ka in SPAN:
            if abs(ka - pa) > 1:
                continue
            for kb in SPAN:
                lhs = lefts(ka, kb)
                rhs = rights(ka, kb)
                blank = jnp.zeros(lhs.shape, jnp.bfloat16)
                rows = jnp.concatenate(
                    [rhs[ka - pa + 1, kb - pb + 1] if abs(kb - pb) <= 1 else blank for pb in SPAN],
                    axis=0,
                )
                term = lax.dot_general(
                    lhs, rows, (((1,), (1,)), ((), ())), preferred_element_type=jnp.float32
                )
                total = term if total is None else total + term
        for pb in SPAN:
            cut = total[:, (pb + 1) * width:(pb + 2) * width]
            emit(pa + 1, pb + 1, cut)


def kernel(counts, orb, pot, den, pattern, ham, mar, pur,
           o_near, v_near, w_near, d0_near, d1_near, m_near, u_near, t0_near, t1_near, first, send, recv):
    width, cells = orb.shape[-2], orb.shape[-1]
    me = (lax.axis_index("gx"), lax.axis_index("yz"))

    def where(da, db):
        return (
            lax.rem(me[0] + da + counts[0], counts[0]),
            lax.rem(me[1] + db + counts[1], counts[1]),
        )

    keep = {
        (a, b): pattern[3 * a + b].astype(jnp.float32) for a in range(3) for b in range(3)
    }
    barrier = pltpu.get_barrier_semaphore()
    for da, db in ((0, 1), (0, -1), (1, 0), (-1, 0)):
        pl.semaphore_signal(barrier, inc=1, device_id=where(da, db), device_id_type=MESH)
    pl.semaphore_wait(barrier, 4)

    used = iter(range(7))

    def halo(own, near, **more):
        at = next(used)
        return Halo(where, own, near, send.at[at], recv.at[at], **more)

    waves = halo(orb, o_near, sign=-1)
    v_own = v_near.at[1, 1]
    v_own[0:1] = pot[0]
    for a in range(3):
        for b in range(3):
            at = 1 + 3 * a + b
            v_own[at:at + 1] = jnp.full((1, cells), keep[a, b], jnp.float32)
    fields = halo(v_own, v_near, whole=True)
    fields.start()
    waves.start()
    d_own = d0_near.at[1, 1]
    for a in range(3):
        for b in range(3):
            d_own[a, b] = (den[a, b].astype(jnp.float32) * keep[a, b]).astype(jnp.bfloat16)
    density = halo(d_own, d0_near)
    density.start_far()
    def region(ka, kb):
        return orb if (ka, kb) == (0, 0) else o_near.at[ka + 1, kb + 1]

    def prepare(regions):
        lane = lax.broadcasted_iota(jnp.int32, (width, 128), 1)
        for ka, kb in regions:
            src = region(ka, kb)
            field = pot[0] if (ka, kb) == (0, 0) else v_near[ka + 1, kb + 1, 0:1]
            for la in SPAN:
                for lb in SPAN:
                    if abs(ka - la) > 1 or abs(kb - lb) > 1:
                        continue
                    value = src[la + 1, lb + 1].astype(jnp.float32)
                    dst = w_near.at[ka + 1, kb + 1, la + 1, lb + 1]
                    dst[:, :cells] = (value * field).astype(jnp.bfloat16)
                    for line in range(cells // 128):
                        piece = value[:, line * 128:(line + 1) * 128]
                        ahead = pltpu.roll(piece, 127, 1)
                        step = jnp.where(lane < 127, ahead - piece, 0.0)
                        at = cells + line * 128
                        dst[:, at:at + 128] = step.astype(jnp.bfloat16)

    fields.relay()
    prepare([(0, 0)])
    waves.relay()
    density.start_near()
    prepare([(0, 1), (0, -1)])
    waves.finish()

    m_own, u_own = m_near.at[1, 1], u_near.at[1, 1]

    def put_margin(a, b, value):
        kept = value * keep[a, b]
        mar[a, b] = kept
        m_own[a, b] = kept.astype(jnp.bfloat16)
        u_own[a, b] = value.astype(jnp.bfloat16)

    overlap(lambda ka, kb: region(ka, kb)[ka + 1, kb + 1], region, width, put_margin)
    margin = halo(u_own, u_near, slim=True)
    margin.start()
    fields.finish()
    density.relay()
    margin.relay()

    def h_left(ka, kb):
        half = w_near[ka + 1, kb + 1, ka + 1, kb + 1][:, cells:] * 0.5
        return jnp.concatenate([region(ka, kb)[ka + 1, kb + 1], half.astype(jnp.bfloat16)], axis=1)

    def put_ham(a, b, value):
        ham[a, b] = value * keep[a, b]

    def complete(local):
        for ja in SPAN:
            for jb in SPAN:
                for ka in SPAN:
                    for kb in SPAN:
                        pa, pb = ka - ja, kb - jb
                        if (ja, jb) == (0, 0) or abs(pa) > 1 or abs(pb) > 1:
                            continue
                        if local != ((ka, kb) == (0, 0)):
                            continue
                        sent = (pa, pb) == (0, 0) or ja == 0 or (jb == 0 and pa == 0)
                        if sent and not local:
                            block = u_near[ja + 1, jb + 1, pa + 1, pb + 1].astype(jnp.float32)
                        else:
                            block = u_near[ka + 1, kb + 1, 1 - pa, 1 - pb].astype(jnp.float32).T
                        at = 1 + 3 * (pa + 1) + pb + 1
                        kept = block * v_near[ja + 1, jb + 1, at:at + 1, :width]
                        m_near[ja + 1, jb + 1, pa + 1, pb + 1] = kept.astype(jnp.bfloat16)

    complete(True)
    margin.finish()
    complete(False)
    density.finish()

    def put_first(a, b, value):
        first[a, b] = value.astype(jnp.bfloat16)

    started = [waves, fields, density, margin]
    nears = ((d0_near, t0_near), (d1_near, t1_near))
    for turn, (d_near, t_near) in enumerate(nears):
        d_row, t_row = d_near.at[1, 1], t_near.at[1, 1]
        product(d_row, m_own, m_near, keep, put_first)
        if turn:
            rows.relay()
            overlap(h_left, lambda ka, kb: w_near.at[ka + 1, kb + 1], width, put_ham)
            rows.finish()

        def put_third(a, b, value):
            pur[a, b] = 3.0 * value
            t_row[a, b] = value.astype(jnp.bfloat16)

        product(first, d_row, d_near, keep, put_third)
        cubic = halo(t_row, t_near)
        cubic.start()
        cubic.relay()
        if not turn:
            prepare([(ka, kb) for ka in (-1, 1) for kb in SPAN])
        cubic.finish()
        started.append(cubic)
        after = nears[turn + 1][0].at[1, 1] if turn + 1 < len(nears) else None

        def put_fifth(a, b, value):
            result = pur[a, b] - 2.0 * value
            pur[a, b] = result
            if after is not None:
                after[a, b] = result.astype(jnp.bfloat16)

        product(first, t_row, t_near, keep, put_fifth)
        if after is not None:
            rows = halo(after, nears[turn + 1][0])
            rows.start()
            started.append(rows)
    for one in started:
        one.drain()


def body(counts, orbitals, potential, density, pattern):
    width, cells = orbitals.shape[3], orbitals.shape[4]
    near = pltpu.VMEM((3, 3, 3, 3, width, width), jnp.bfloat16)
    blocks = jax.ShapeDtypeStruct((3, 3, width, width), jnp.float32)
    vmem = pl.BlockSpec(memory_space=pltpu.VMEM)
    outs = pl.pallas_call(
        functools.partial(kernel, counts),
        out_shape=(blocks,) * 3,
        in_specs=[vmem, vmem, vmem, pl.BlockSpec(memory_space=pltpu.SMEM)],
        out_specs=(vmem,) * 3,
        scratch_shapes=[
            pltpu.VMEM((3, 3, 3, 3, width, cells), jnp.bfloat16),
            pltpu.VMEM((3, 3, 16, cells), jnp.float32),
            pltpu.VMEM((3, 3, 3, 3, width, 2 * cells), jnp.bfloat16),
            near, near, near, near, near, near,
            pltpu.VMEM((3, 3, width, width), jnp.bfloat16),
            pltpu.SemaphoreType.DMA((7, 16)),
            pltpu.SemaphoreType.DMA((7, 16)),
        ],
        compiler_params=pltpu.CompilerParams(
            collective_id=0, has_side_effects=True, vmem_limit_bytes=44 * 2**20
        ),
    )(
        orbitals.reshape(3, 3, width, cells),
        potential.reshape(1, 1, cells),
        density.reshape(3, 3, width, width),
        pattern.reshape(9),
    )
    return tuple(out.reshape(1, 1, 9, width, width) for out in outs)


def solution(mesh):
    rows = P("gx", "yz", None, None, None)
    flat = P("gx", "yz", None)
    return jax.shard_map(
        functools.partial(body, (mesh.shape["gx"], mesh.shape["yz"])),
        mesh=mesh,
        in_specs=(rows, flat, rows, flat),
        out_specs=(rows,) * 3,
        check_vma=False,
    )
```
